128 devices in a mesh: sec: 2 (over z_lo), tile: 64 (over y, z_hi, x, core).
Axes of the slice: x: 4, y: 4, z: 4 (z_hi: 2, z_lo: 2; z = z_hi * 2 + z_lo), core: 2. Of those that a mesh axis runs over, the one named last changes fastest.
Arguments:
- atmosphere: bfloat16 [128, 360, 384], P(('sec', 'tile')), may hold values from -6 to 6
- ocean_state: bfloat16 [512, 1440, 128], P('tile', 'sec'), may hold values from -6 to 6
- land_mask: int32 [512, 1440], P('tile', 'sec'), may hold values 0 or 1
- crossing_bands: int32 [64, 4], P('tile'), may hold values from 0 to 127, as said below
- ocean_regrid: float32 [64, 4, 8, 1], P('tile'), may hold values from 0 to 1, as said below
- atmosphere_regrid: float32 [64, 4, 1, 8], P('tile'), may hold values from 0 to 1, as said below
- surface_read: bfloat16 [128], replicated, may hold values from -0.5 to 0.5
- surface_embed: float32 [384], replicated, may hold values from -4 to 4
- flux_read: bfloat16 [384, 8], replicated, may hold values from -0.3125 to 0.3125
- flux_embed: bfloat16 [8, 128], replicated, may hold values from -2 to 2
- legendre_forward: bfloat16 [128, 128, 128], P(('sec', 'tile')), may hold values from -0.5 to 0.5
- legendre_inverse: bfloat16 [128, 128, 128], P(('sec', 'tile')), may hold values from -0.5 to 0.5
- spectral_mix: bfloat16 [2, 384, 384], replicated, may hold values from -0.3125 to 0.3125
- conv_kernel: bfloat16 [2, 7, 7, 128], replicated, may hold values from -0.875 to 0.875
- norm_gain: float32 [2, 128], replicated, may hold values from 0.1 to 1.9
- expand_weight: bfloat16 [2, 128, 512], replicated, may hold values from -0.5 to 0.5
- project_weight: bfloat16 [2, 512, 128], replicated, may hold values from -0.25 to 0.25
- atmosphere_cotangent: bfloat16 [128, 360, 384], P(('sec', 'tile')), may hold values from -6 to 6
- ocean_cotangent: bfloat16 [512, 1440, 128], P('tile', 'sec'), may hold values from -6 to 6
Outputs:
- atmosphere_next: bfloat16 [128, 360, 384], P(('sec', 'tile'))
- ocean_next: bfloat16 [512, 1440, 128], P('tile', 'sec')
- atmosphere_grad: float32 [128, 360, 384], P(('sec', 'tile'))
- ocean_grad: float32 [512, 1440, 128], P('tile', 'sec')
The draws below stay inside these ranges and needn't reach their ends.
Inputs may be any that keep to these rules, and one draw needn't show every extreme that they name: `crossing_bands`: row j lists between 1 and 4 consecutive distinct atmosphere bands, then repeats its last band; some row lists 4. Its first band is j * 2 - 1, j * 2 or j * 2 + 1, raised to 0 or lowered as far as needed for the list to end at band 128 - 1 at most. `ocean_regrid`: zero in the repeated slots of crossing_bands; the entries of each ocean row sum to one. `atmosphere_regrid`: zero in the repeated slots of crossing_bands.
All inputs are finite; a program needn't handle non-finite values. No bound on the sum of `land_mask` on one device may be relied on, other than what follows from the above.
Results may differ from the reference program's by a relative error of at most 0.008.
Values may be sent and summed in bfloat16 or wider, within the bound.
No kernel may reach another device: no remote copies, remote signals or barrier semaphores. Data moves between devices by JAX's collectives and lax.ppermute only.
A program may use at most 128 MiB of HBM per device.

```python
import jax
import jax.numpy as jnp
from jax import lax

C = 384
ALON = 360
MODES = 128
F = 8
OC = 128
OHID = 512
KS = 7
LAYERS = 2
PEERS = 4
ALAT_DEV = 1
OLAT_DEV = 8
BANDS = 128
GROUPS = 64
ALAT = 128
OLAT = 512
OLON = 1440


def crossing_layout(key):
    base = jax.random.fold_in(key, 17)
    count_key, step_key = jax.random.split(base)
    group_index = jnp.arange(GROUPS, dtype=jnp.int32)
    counts = jax.random.randint(count_key, (GROUPS,), 1, PEERS + 1).astype(jnp.int32)
    counts = jnp.where(group_index == GROUPS // 2, PEERS, counts)
    wiggle = jax.random.randint(step_key, (GROUPS,), -1, 2).astype(jnp.int32)
    first = group_index * (BANDS // GROUPS) + wiggle
    first = jnp.minimum(jnp.maximum(first, 0), BANDS - counts)
    slot = jnp.arange(PEERS, dtype=jnp.int32)
    listed = first[:, None] + jnp.minimum(slot[None, :], counts[:, None] - 1)
    valid = (slot[None, :] < counts[:, None]).astype(jnp.float32)
    return (listed.astype(jnp.int32), valid)


def positive_weights(key, shape):
    raw = jax.random.uniform(key, shape, jnp.float32, 0.2, 1.0)
    return raw


def draw_crossing_bands(key, part):
    return crossing_layout(key)[0]


def draw_ocean_regrid(key, part):
    listed, valid = crossing_layout(key)
    raw = positive_weights(jax.random.fold_in(key, 29), (GROUPS, PEERS, OLAT_DEV, ALAT_DEV))
    raw = raw * valid[:, :, None, None]
    return raw / jnp.sum(raw, axis=(1, 3), keepdims=True)


def draw_atmosphere_regrid(key, part):
    listed, valid = crossing_layout(key)
    raw = positive_weights(jax.random.fold_in(key, 31), (GROUPS, PEERS, ALAT_DEV, OLAT_DEV))
    return raw * valid[:, :, None, None] / OLAT_DEV


def touch_ends(array, own_key, smallest, largest):
    place = [jax.random.randint(jax.random.fold_in(own_key, axis), (), 0, length) for axis, length in enumerate(array.shape)]
    widest = array.shape.index(max(array.shape))
    beside = place[:widest] + [(place[widest] + 1) % array.shape[widest]] + place[widest + 1:]
    return array.at[tuple(place)].set(smallest).at[tuple(beside)].set(largest)


def shard_levels(rng, shape, cuts, least, high):
    def one(axis_at, shards_of):
        steps = jax.random.uniform(jax.random.fold_in(jax.random.fold_in(rng, 6), axis_at), (shards_of,), jnp.float32, least / len(cuts), high / len(cuts))
        return jnp.repeat(jnp.exp(steps), shape[axis_at] // shards_of).reshape((-1,) + (1,) * (len(shape) - axis_at - 1))

    loudness = one(*cuts[0])
    for cut in cuts[1:]:
        loudness = loudness * one(*cut)
    return loudness


def centred(stream_key, shape, deviation, limit, cuts=(), kind=jnp.bfloat16):
    entries = jax.random.normal(stream_key, shape, jnp.float32) * deviation
    if len(cuts) > 0:
        entries = shard_levels(stream_key, shape, cuts, -0.22, 0.18) * entries
    return jnp.clip(entries, min=-limit, max=limit).astype(kind)


def setup_inputs(seed: int = 0) -> dict:
    arg_keys = jax.random.split(jax.random.key(seed), 20)
    return {
        "atmosphere": centred(arg_keys[0], (ALAT, ALON, C), 1.0, 6.0, ((0, 128),)),
        "ocean_state": centred(arg_keys[1], (OLAT, OLON, OC), 1.0, 6.0, ((0, 64), (1, 2))),
        "land_mask": touch_ends((jax.random.randint(arg_keys[2], (OLAT, OLON), 0, 10) < 7).astype(jnp.int32), jax.random.fold_in(arg_keys[2], 1), 0, 1),
        "crossing_bands": draw_crossing_bands(jax.random.fold_in(arg_keys[19], 71), 0),
        "ocean_regrid": draw_ocean_regrid(jax.random.fold_in(arg_keys[19], 71), 0),
        "atmosphere_regrid": draw_atmosphere_regrid(jax.random.fold_in(arg_keys[19], 71), 0),
        "surface_read": centred(arg_keys[6], (OC,), OC ** -0.5, 0.5),
        "surface_embed": centred(arg_keys[7], (C,), 1.0, 4.0, (), jnp.float32),
        "flux_read": centred(arg_keys[8], (C, F), C ** -0.5, 0.3125),
        "flux_embed": centred(arg_keys[9], (F, OC), F ** -0.5, 2.0),
        "legendre_forward": centred(arg_keys[10], (MODES, ALAT, ALAT), ALAT ** -0.5, 0.5, ((0, 128),)),
        "legendre_inverse": centred(arg_keys[11], (MODES, ALAT, ALAT), ALAT ** -0.5, 0.5, ((0, 128),)),
        "spectral_mix": centred(arg_keys[12], (2, C, C), C ** -0.5, 0.3125),
        "conv_kernel": centred(arg_keys[13], (LAYERS, KS, KS, OC), (KS * KS) ** -0.5, 0.875),
        "norm_gain": jnp.clip(1.0 + 0.18 * jax.random.normal(arg_keys[14], (LAYERS, OC), jnp.float32), 0.1, 1.9),
        "expand_weight": centred(arg_keys[15], (LAYERS, OC, OHID), OC ** -0.5, 0.5),
        "project_weight": centred(arg_keys[16], (LAYERS, OHID, OC), OHID ** -0.5, 0.25),
        "atmosphere_cotangent": centred(arg_keys[17], (ALAT, ALON, C), 1.0, 6.0, ((0, 128),)),
        "ocean_cotangent": centred(arg_keys[18], (OLAT, OLON, OC), 1.0, 6.0, ((0, 64), (1, 2))),
    }


def wave_table(lon_count, mode_count):
    longitude = jnp.arange(lon_count, dtype=jnp.int32)
    wavenumber = jnp.arange(mode_count, dtype=jnp.int32)
    phase = (longitude[:, None] * wavenumber[None, :] % lon_count).astype(jnp.float32) * (2.0 * jnp.pi / lon_count)
    scaled = jnp.stack([jnp.cos(phase), -jnp.sin(phase)], axis=2) * jnp.sqrt(jnp.float32(2.0 / lon_count))
    return scaled.reshape(lon_count, 2 * mode_count).astype(jnp.bfloat16)

def depthwise(window, kernel):
    radius = kernel.shape[0] // 2
    height = window.shape[0] - 2 * radius
    extent = window.shape[1]
    wide = jnp.concatenate([window[:, extent - radius:], window, window[:, :radius]], axis=1).astype(jnp.float32)
    weights = kernel.astype(jnp.float32)
    total = jnp.zeros((height, extent, window.shape[2]), jnp.float32)
    for shift_row in range(kernel.shape[0]):
        for shift_col in range(kernel.shape[1]):
            total = total + wide[shift_row:shift_row + height, shift_col:shift_col + extent] * weights[shift_row, shift_col]
    return total

def cell_forward(hidden, gain, expand, project):
    center = hidden - lax.optimization_barrier(jnp.mean(hidden, axis=-1, keepdims=True))
    inverse_std = lax.rsqrt(lax.optimization_barrier(jnp.mean(center * center, axis=-1, keepdims=True)) + 1e-06)
    normed = (center * inverse_std * gain).astype(jnp.bfloat16)
    before = jnp.dot(normed, expand, preferred_element_type=jnp.float32)
    active = jax.nn.gelu(before).astype(jnp.bfloat16)
    return jnp.dot(active, project, preferred_element_type=jnp.float32)

def cell_backward(hidden, gain, expand, project, mask_value, cotangent):
    center = hidden - lax.optimization_barrier(jnp.mean(hidden, axis=-1, keepdims=True))
    inverse_std = lax.rsqrt(lax.optimization_barrier(jnp.mean(center * center, axis=-1, keepdims=True)) + 1e-06)
    unit = center * inverse_std
    normed = (unit * gain).astype(jnp.bfloat16)
    before = jnp.dot(normed, expand, preferred_element_type=jnp.float32)
    masked = (mask_value[:, :, None] * cotangent).astype(jnp.bfloat16)
    active_adjoint = jnp.dot(masked, project.T, preferred_element_type=jnp.float32)
    _, gelu_back = jax.vjp(jax.nn.gelu, before)
    before_adjoint = gelu_back(active_adjoint)[0].astype(jnp.bfloat16)
    normed_adjoint = jnp.dot(before_adjoint, expand.T, preferred_element_type=jnp.float32)
    scaled = normed_adjoint * gain
    result = inverse_std * (scaled - lax.optimization_barrier(jnp.mean(scaled, axis=-1, keepdims=True)) - unit * lax.optimization_barrier(jnp.mean(scaled * unit, axis=-1, keepdims=True)))
    return result.astype(jnp.bfloat16)

def ocean_matrix(bands_row, blocks, lat_count):
    lat_band = blocks.shape[2]
    index = bands_row[:, None] * lat_band + jnp.arange(lat_band, dtype=jnp.int32)[None, :]
    onehot = (index[:, :, None] == jnp.arange(lat_count, dtype=jnp.int32)[None, None, :]).astype(jnp.float32)
    return jnp.einsum('poi,pia->oa', blocks, onehot, precision=lax.Precision.HIGHEST)

def atmosphere_matrix(bands_row, blocks, lat_count):
    lat_band = blocks.shape[1]
    index = bands_row[:, None] * lat_band + jnp.arange(lat_band, dtype=jnp.int32)[None, :]
    onehot = (index[:, :, None] == jnp.arange(lat_count, dtype=jnp.int32)[None, None, :]).astype(jnp.float32)
    return jnp.einsum('pio,pia->ao', blocks, onehot, precision=lax.Precision.HIGHEST)

def mix_complex(coefficient, mix_real, mix_imag):
    real_part = coefficient[:, :, 0].astype(jnp.float32)
    imag_part = coefficient[:, :, 1].astype(jnp.float32)
    first = mix_real.astype(jnp.float32)
    second = mix_imag.astype(jnp.float32)
    out_real = jnp.einsum('lmc,cd->lmd', real_part, first) - jnp.einsum('lmc,cd->lmd', imag_part, second)
    out_imag = jnp.einsum('lmc,cd->lmd', imag_part, first) + jnp.einsum('lmc,cd->lmd', real_part, second)
    return jnp.stack([out_real, out_imag], axis=2).astype(jnp.bfloat16)

def spectral_block(spectrum, forward, inverse, mixing):
    lat_count, columns, channels = spectrum.shape
    split = spectrum.reshape(lat_count, columns // 2, 2, channels).astype(jnp.float32)
    coefficient = jnp.einsum('mla,amrc->lmrc', forward.astype(jnp.float32), split).astype(jnp.bfloat16)
    mixed = mix_complex(coefficient, mixing[0], mixing[1])
    returned = jnp.einsum('mal,lmrc->amrc', inverse.astype(jnp.float32), mixed.astype(jnp.float32)).astype(jnp.bfloat16)
    return returned.reshape(lat_count, columns, channels)

def spectral_adjoint(returned_adjoint, forward, inverse, mixing):
    lat_count, columns, channels = returned_adjoint.shape
    split = returned_adjoint.reshape(lat_count, columns // 2, 2, channels).astype(jnp.float32)
    mixed_adjoint = jnp.einsum('mal,amrc->lmrc', inverse.astype(jnp.float32), split).astype(jnp.bfloat16)
    real_part = mixed_adjoint[:, :, 0].astype(jnp.float32)
    imag_part = mixed_adjoint[:, :, 1].astype(jnp.float32)
    first = mixing[0].astype(jnp.float32)
    second = mixing[1].astype(jnp.float32)
    back_real = jnp.einsum('lmd,cd->lmc', real_part, first) + jnp.einsum('lmd,cd->lmc', imag_part, second)
    back_imag = jnp.einsum('lmd,cd->lmc', imag_part, first) - jnp.einsum('lmd,cd->lmc', real_part, second)
    coefficient_adjoint = jnp.stack([back_real, back_imag], axis=2).astype(jnp.bfloat16)
    spectrum_adjoint = jnp.einsum('mla,lmrc->amrc', forward.astype(jnp.float32), coefficient_adjoint.astype(jnp.float32)).astype(jnp.bfloat16)
    return spectrum_adjoint.reshape(lat_count, columns, channels)

def ocean_layer(state, mask_value, kernel, gain, expand, project, band):
    radius = kernel.shape[0] // 2
    padded = jnp.pad(state, ((radius, radius), (0, 0), (0, 0)))
    band_count = state.shape[0] // band

    def one_band(index):
        start = index * band
        window = lax.dynamic_slice_in_dim(padded, start, band + 2 * radius, 0)
        update = cell_forward(depthwise(window, kernel), gain, expand, project)
        own = lax.dynamic_slice_in_dim(state, start, band, 0).astype(jnp.float32)
        weight = lax.dynamic_slice_in_dim(mask_value, start, band, 0)
        return (own + weight[:, :, None] * update).astype(jnp.bfloat16)
    result = lax.map(one_band, jnp.arange(band_count, dtype=jnp.int32))
    return result.reshape(state.shape)

def ocean_layer_adjoint(state, mask_value, kernel, gain, expand, project, cotangent, band):
    radius = kernel.shape[0] // 2
    padded = jnp.pad(state, ((radius, radius), (0, 0), (0, 0)))
    band_count = state.shape[0] // band

    def local_adjoint(index):
        start = index * band
        window = lax.dynamic_slice_in_dim(padded, start, band + 2 * radius, 0)
        hidden = depthwise(window, kernel)
        local_cotangent = lax.dynamic_slice_in_dim(cotangent, start, band, 0)
        weight = lax.dynamic_slice_in_dim(mask_value, start, band, 0)
        return cell_backward(hidden, gain, expand, project, weight, local_cotangent)
    hidden_adjoint = lax.map(local_adjoint, jnp.arange(band_count, dtype=jnp.int32)).reshape(state.shape)
    padded_adjoint = jnp.pad(hidden_adjoint, ((radius, radius), (0, 0), (0, 0)))
    flipped = kernel[::-1, ::-1]

    def spread(index):
        start = index * band
        window = lax.dynamic_slice_in_dim(padded_adjoint, start, band + 2 * radius, 0)
        return depthwise(window, flipped)
    spreads = lax.map(spread, jnp.arange(band_count, dtype=jnp.int32)).reshape(state.shape)
    return cotangent + spreads

def reference(atmosphere, ocean_state, land_mask, crossing_bands, ocean_regrid, atmosphere_regrid, surface_read, surface_embed, flux_read, flux_embed, legendre_forward, legendre_inverse, spectral_mix, conv_kernel, norm_gain, expand_weight, project_weight, atmosphere_cotangent, ocean_cotangent):
    group_total = crossing_bands.shape[0]
    lat_count, lon_count, channels = atmosphere.shape
    ocean_rows, ocean_lon, ocean_channels = ocean_state.shape
    band = ocean_rows // group_total
    ratio = ocean_lon // lon_count
    flux_count = flux_read.shape[1]
    highest = lax.Precision.HIGHEST
    to_ocean = jax.vmap(lambda row, blocks: ocean_matrix(row, blocks, lat_count))(crossing_bands, ocean_regrid)
    to_ocean = to_ocean.reshape(ocean_rows, lat_count)
    to_atmosphere = jax.vmap(lambda row, blocks: atmosphere_matrix(row, blocks, lat_count))(crossing_bands, atmosphere_regrid)
    to_atmosphere = jnp.transpose(to_atmosphere, (1, 0, 2)).reshape(lat_count, ocean_rows)
    mask_value = land_mask.astype(jnp.float32)
    surface = jnp.dot(ocean_state, surface_read, preferred_element_type=jnp.float32)
    coarse = lax.optimization_barrier(jnp.mean((mask_value * surface).reshape(ocean_rows, lon_count, ratio), axis=2))
    surface_atmosphere = jnp.dot(to_atmosphere, coarse, precision=highest)
    mixed_input = (atmosphere.astype(jnp.float32) + surface_atmosphere[:, :, None] * surface_embed[None, None, :]).astype(jnp.bfloat16)
    table = wave_table(lon_count, legendre_forward.shape[0]).astype(jnp.float32)
    spectrum = jnp.einsum('gk,agc->akc', table, mixed_input.astype(jnp.float32)).astype(jnp.bfloat16)
    returned = spectral_block(spectrum, legendre_forward, legendre_inverse, spectral_mix)
    response = jnp.einsum('gk,akc->agc', table, returned.astype(jnp.float32))
    atmosphere_next = (mixed_input.astype(jnp.float32) + jax.nn.gelu(response)).astype(jnp.bfloat16)
    flux = jnp.einsum('agc,cf->agf', atmosphere.astype(jnp.float32), flux_read.astype(jnp.float32))
    flux_ocean = jnp.dot(to_ocean, flux.reshape(lat_count, lon_count * flux_count), precision=highest)
    forcing_coarse = jnp.einsum('ogf,fc->ogc', flux_ocean.reshape(ocean_rows, lon_count, flux_count), flux_embed.astype(jnp.float32), precision=highest)
    forcing = jnp.broadcast_to(forcing_coarse[:, :, None, :], (ocean_rows, lon_count, ratio, ocean_channels)).reshape(ocean_rows, ocean_lon, ocean_channels)
    state = (ocean_state.astype(jnp.float32) + mask_value[:, :, None] * forcing).astype(jnp.bfloat16)
    states = []
    for layer in range(conv_kernel.shape[0]):
        states.append(state)
        state = ocean_layer(state, mask_value, conv_kernel[layer], norm_gain[layer], expand_weight[layer], project_weight[layer], band)
    ocean_next = state
    cotangent = ocean_cotangent.astype(jnp.float32)
    for layer in range(conv_kernel.shape[0] - 1, -1, -1):
        cotangent = ocean_layer_adjoint(states[layer], mask_value, conv_kernel[layer], norm_gain[layer], expand_weight[layer], project_weight[layer], cotangent, band)
    forcing_adjoint = (mask_value[:, :, None] * cotangent).reshape(ocean_rows, lon_count, ratio, ocean_channels).sum(axis=2)
    flux_ocean_adjoint = jnp.einsum('ogc,fc->ogf', forcing_adjoint, flux_embed.astype(jnp.float32), precision=highest)
    flux_adjoint = jnp.dot(to_ocean.T, flux_ocean_adjoint.reshape(ocean_rows, lon_count * flux_count), precision=highest)
    flux_adjoint = flux_adjoint.reshape(lat_count, lon_count, flux_count)
    from_flux = jnp.einsum('agf,cf->agc', flux_adjoint, flux_read.astype(jnp.float32), precision=highest)
    atmosphere_adjoint = atmosphere_cotangent.astype(jnp.float32)
    _, gelu_back = jax.vjp(jax.nn.gelu, response)
    response_adjoint = gelu_back(atmosphere_adjoint)[0].astype(jnp.bfloat16)
    returned_adjoint = jnp.einsum('gk,agc->akc', table, response_adjoint.astype(jnp.float32)).astype(jnp.bfloat16)
    spectrum_adjoint = spectral_adjoint(returned_adjoint, legendre_forward, legendre_inverse, spectral_mix)
    input_adjoint = atmosphere_adjoint + jnp.einsum('gk,akc->agc', table, spectrum_adjoint.astype(jnp.float32))
    atmosphere_grad = input_adjoint + from_flux
    surface_adjoint = jnp.einsum('agc,c->ag', input_adjoint, surface_embed, precision=highest)
    coarse_adjoint = jnp.dot(to_atmosphere.T, surface_adjoint, precision=highest)
    widened = jnp.broadcast_to(coarse_adjoint[:, :, None], (ocean_rows, lon_count, ratio)).reshape(ocean_rows, ocean_lon)
    surface_grad = mask_value * widened / ratio
    ocean_grad = cotangent + surface_grad[:, :, None] * surface_read.astype(jnp.float32)[None, None, :]
    return (atmosphere_next, ocean_next, atmosphere_grad, ocean_grad)
```

```python
import jax
import jax.numpy as jnp
from jax import lax
from jax.sharding import Mesh
from jax.sharding import PartitionSpec as P

SEC_TILE = ("sec", "tile_0", "tile_1", "tile_2", "tile_3")
TILE = ("tile_0", "tile_1", "tile_2", "tile_3")


def in_blocks(x, dim, size):
    lengths = x.shape
    blocks = x.reshape(*lengths[:dim], size, lengths[dim] // size, *lengths[dim + 1 :])
    return jnp.moveaxis(blocks, dim, 0)


def laid_out(blocks, dim):
    lengths = list(blocks.shape[1:])
    lengths[dim] *= blocks.shape[0]
    return jnp.moveaxis(blocks, 0, dim).reshape(lengths)


def turned_blocks(blocks, axes, sequence):
    lengths = [lax.axis_size(a) for a in axes]
    blocks = blocks.reshape(*lengths, *blocks.shape[1:])
    for k in sequence:
        blocks = lax.all_to_all(blocks, axes[k], split_axis=k, concat_axis=k, tiled=True)
    return blocks.reshape(-1, *blocks.shape[len(axes) :])


def two_step_exchange(x, groups, sequence, split_dim, concat_dim):
    size = lax.axis_size(groups[0]) * lax.axis_size(groups[1])
    blocks = in_blocks(x, split_dim, size)
    return laid_out(turned_blocks(blocks, groups, sequence), concat_dim)


def with_halo(x, sides, width, wrap):
    for axis, dim in sides:
        size, length = (lax.axis_size(axis), x.shape[dim])
        up = [(i, (i + 1) % size) for i in range(size if wrap else size - 1)]
        down = [(j, i) for i, j in up]
        last = lax.slice_in_dim(x, length - width, length, axis=dim)
        first = lax.slice_in_dim(x, 0, width, axis=dim)
        before = lax.ppermute(last, axis, up)
        after = lax.ppermute(first, axis, down)
        x = jnp.concatenate([before, x, after], axis=dim)
    return x


def wave_table(lon_count, mode_count):
    longitude = jnp.arange(lon_count, dtype=jnp.int32)
    wavenumber = jnp.arange(mode_count, dtype=jnp.int32)
    phase = (longitude[:, None] * wavenumber[None, :] % lon_count).astype(jnp.float32) * (
        2.0 * jnp.pi / lon_count
    )
    scaled = jnp.stack([jnp.cos(phase), -jnp.sin(phase)], axis=2) * jnp.sqrt(
        jnp.float32(2.0 / lon_count)
    )
    return scaled.reshape(lon_count, 2 * mode_count).astype(jnp.bfloat16)


def depthwise(window, kernel):
    radius = kernel.shape[0] // 2
    height = window.shape[0] - 2 * radius
    extent = window.shape[1] - 2 * radius
    wide = window.astype(jnp.float32)
    weights = kernel.astype(jnp.float32)
    total = jnp.zeros((height, extent, window.shape[2]), jnp.float32)
    for shift_row in range(kernel.shape[0]):
        for shift_col in range(kernel.shape[1]):
            total = (
                total
                + wide[shift_row : shift_row + height, shift_col : shift_col + extent]
                * weights[shift_row, shift_col]
            )
    return total


def cell_forward(hidden, gain, expand, project):
    center = hidden - jnp.mean(hidden, axis=-1, keepdims=True)
    inverse_std = lax.rsqrt(jnp.mean(center * center, axis=-1, keepdims=True) + 1e-06)
    normed = (center * inverse_std * gain).astype(jnp.bfloat16)
    before = jnp.dot(normed, expand, preferred_element_type=jnp.float32)
    active = jax.nn.gelu(before).astype(jnp.bfloat16)
    return jnp.dot(active, project, preferred_element_type=jnp.float32)


def cell_backward(hidden, gain, expand, project, mask_value, cotangent):
    center = hidden - jnp.mean(hidden, axis=-1, keepdims=True)
    inverse_std = lax.rsqrt(jnp.mean(center * center, axis=-1, keepdims=True) + 1e-06)
    unit = center * inverse_std
    normed = (unit * gain).astype(jnp.bfloat16)
    before = jnp.dot(normed, expand, preferred_element_type=jnp.float32)
    masked = (mask_value[:, :, None] * cotangent).astype(jnp.bfloat16)
    active_adjoint = jnp.dot(masked, project.T, preferred_element_type=jnp.float32)
    _, gelu_back = jax.vjp(jax.nn.gelu, before)
    before_adjoint = gelu_back(active_adjoint)[0].astype(jnp.bfloat16)
    normed_adjoint = jnp.dot(before_adjoint, expand.T, preferred_element_type=jnp.float32)
    scaled = normed_adjoint * gain
    result = inverse_std * (
        scaled
        - jnp.mean(scaled, axis=-1, keepdims=True)
        - unit * jnp.mean(scaled * unit, axis=-1, keepdims=True)
    )
    return result.astype(jnp.bfloat16)


def mix_complex(coefficient, mix_real, mix_imag):
    real_part = coefficient[:, :, 0]
    imag_part = coefficient[:, :, 1]
    out_real = jnp.einsum(
        "lmc,cd->lmd", real_part, mix_real, preferred_element_type=jnp.float32
    ) - jnp.einsum("lmc,cd->lmd", imag_part, mix_imag, preferred_element_type=jnp.float32)
    out_imag = jnp.einsum(
        "lmc,cd->lmd", imag_part, mix_real, preferred_element_type=jnp.float32
    ) + jnp.einsum("lmc,cd->lmd", real_part, mix_imag, preferred_element_type=jnp.float32)
    return jnp.stack([out_real, out_imag], axis=2).astype(jnp.bfloat16)


def spectral_block(spectrum, forward, inverse, mixing):
    lat_count, columns, channels = spectrum.shape
    split = spectrum.reshape(lat_count, columns // 2, 2, channels)
    coefficient = jnp.einsum(
        "mla,amrc->lmrc", forward, split, preferred_element_type=jnp.float32
    ).astype(jnp.bfloat16)
    mixed = mix_complex(coefficient, mixing[0], mixing[1])
    returned = jnp.einsum(
        "mal,lmrc->amrc", inverse, mixed, preferred_element_type=jnp.float32
    ).astype(jnp.bfloat16)
    return returned.reshape(lat_count, columns, channels)


def spectral_adjoint(returned_adjoint, forward, inverse, mixing):
    lat_count, columns, channels = returned_adjoint.shape
    split = returned_adjoint.reshape(lat_count, columns // 2, 2, channels)
    mixed_adjoint = jnp.einsum(
        "mal,amrc->lmrc", inverse, split, preferred_element_type=jnp.float32
    ).astype(jnp.bfloat16)
    real_part = mixed_adjoint[:, :, 0]
    imag_part = mixed_adjoint[:, :, 1]
    back_real = jnp.einsum(
        "lmd,cd->lmc", real_part, mixing[0], preferred_element_type=jnp.float32
    ) + jnp.einsum("lmd,cd->lmc", imag_part, mixing[1], preferred_element_type=jnp.float32)
    back_imag = jnp.einsum(
        "lmd,cd->lmc", imag_part, mixing[0], preferred_element_type=jnp.float32
    ) - jnp.einsum("lmd,cd->lmc", real_part, mixing[1], preferred_element_type=jnp.float32)
    coefficient_adjoint = jnp.stack([back_real, back_imag], axis=2).astype(jnp.bfloat16)
    spectrum_adjoint = jnp.einsum(
        "mla,lmrc->amrc", forward, coefficient_adjoint, preferred_element_type=jnp.float32
    ).astype(jnp.bfloat16)
    return spectrum_adjoint.reshape(lat_count, columns, channels)


def to_modes(values):
    return two_step_exchange(
        values, (("sec", "tile_0", "tile_1", "tile_2"), "tile_3"), (1, 0), 1, 0
    )


def to_bands(values):
    return lax.all_to_all(values, SEC_TILE, split_axis=0, concat_axis=1, tiled=True)


def rims(values, width):
    with_rows = with_halo(values, ((TILE, 0),), width, False)
    return with_halo(with_rows, (("sec", 1),), width, True)


def half_routes(tiles):
    bands = 2 * tiles
    straight = [(a, (a % 2) * tiles + a // 2) for a in range(bands)]
    crossed = [(a, (1 - a % 2) * tiles + a // 2) for a in range(bands)]
    return straight, crossed


def back(pairs):
    return [(j, i) for i, j in pairs]


def shift_tiles(values, step, tiles):
    pairs = [
        (s * tiles + j, s * tiles + j + step)
        for s in range(2)
        for j in range(tiles)
        if 0 <= j + step < tiles
    ]
    return lax.ppermute(values, SEC_TILE, pairs)


def window_matrix(bands_row, blocks, tiles):
    base = 2 * lax.axis_index(TILE) - 2
    onehot = (
        (bands_row - base)[:, None] == jnp.arange(8, dtype=jnp.int32)[None, :]
    ).astype(jnp.float32)
    return jnp.sum(blocks[:, :, None] * onehot[:, None, :], axis=0)


def rows_to_windows(values, tiles):
    lon = values.shape[0]
    halves = values.reshape(2, lon // 2, *values.shape[1:])
    odd = lax.axis_index(SEC_TILE) % 2 == 1
    straight, crossed = half_routes(tiles)
    first = lax.ppermute(jnp.where(odd, halves[1], halves[0]), SEC_TILE, straight)
    second = lax.ppermute(jnp.where(odd, halves[0], halves[1]), SEC_TILE, crossed)
    east = lax.axis_index("sec") == 1
    pair = jnp.stack([jnp.where(east, second, first), jnp.where(east, first, second)])
    parts = [
        shift_tiles(pair, 1, tiles),
        pair,
        shift_tiles(pair, -1, tiles),
        shift_tiles(pair, -2, tiles),
    ]
    return jnp.concatenate(parts, axis=0)


def windows_to_rows(parts, tiles):
    pair = (
        parts[2:4]
        + shift_tiles(parts[0:2], -1, tiles)
        + shift_tiles(parts[4:6], 1, tiles)
        + shift_tiles(parts[6:8], 2, tiles)
    )
    east = lax.axis_index("sec") == 1
    straight, crossed = half_routes(tiles)
    first = lax.ppermute(jnp.where(east, pair[1], pair[0]), SEC_TILE, back(straight))
    second = lax.ppermute(jnp.where(east, pair[0], pair[1]), SEC_TILE, back(crossed))
    odd = lax.axis_index(SEC_TILE) % 2 == 1
    return jnp.concatenate([jnp.where(odd, second, first), jnp.where(odd, first, second)])


def per_device(
    atmosphere,
    ocean_state,
    land_mask,
    crossing_bands,
    ocean_regrid,
    atmosphere_regrid,
    surface_read,
    surface_embed,
    flux_read,
    flux_embed,
    legendre_forward,
    legendre_inverse,
    spectral_mix,
    conv_kernel,
    norm_gain,
    expand_weight,
    project_weight,
    atmosphere_cotangent,
    ocean_cotangent,
):
    band_total = lax.axis_size(SEC_TILE)
    lat_rows, lon_count, channels = atmosphere.shape
    lat_count = lat_rows * band_total
    ocean_rows, ocean_lon, ocean_channels = ocean_state.shape
    half = lon_count // lax.axis_size("sec")
    ratio = ocean_lon // half
    flux_count = flux_read.shape[1]
    radius = conv_kernel.shape[1] // 2
    layer_count = conv_kernel.shape[0]
    highest = lax.Precision.HIGHEST
    mask_value = land_mask.astype(jnp.float32)
    tiles = lax.axis_size(TILE)
    to_ocean = window_matrix(crossing_bands[0], ocean_regrid[0, :, :, 0], tiles)
    from_ocean = window_matrix(crossing_bands[0], atmosphere_regrid[0, :, 0, :], tiles)
    surface = jnp.dot(ocean_state, surface_read, preferred_element_type=jnp.float32)
    coarse = jnp.mean((mask_value * surface).reshape(ocean_rows, half, ratio), axis=2)
    surface_atmosphere = windows_to_rows(
        jnp.sum(from_ocean[:, :, None] * coarse[:, None, :], axis=0), tiles
    )[None]
    flux = jnp.einsum("agc,cf->agf", atmosphere, flux_read, preferred_element_type=jnp.float32)
    flux_window = rows_to_windows(flux[0], tiles)
    flux_ocean = jnp.dot(
        to_ocean, flux_window.reshape(flux_window.shape[0], half * flux_count), precision=highest
    )
    mixed_input = (
        atmosphere.astype(jnp.float32)
        + surface_atmosphere[:, :, None] * surface_embed[None, None, :]
    ).astype(jnp.bfloat16)
    table = wave_table(lon_count, legendre_forward.shape[0] * band_total)
    spectrum = jnp.einsum(
        "gk,agc->akc", table, mixed_input, preferred_element_type=jnp.float32
    ).astype(jnp.bfloat16)
    returned = to_bands(
        spectral_block(to_modes(spectrum), legendre_forward, legendre_inverse, spectral_mix)
    )
    response = jnp.einsum("gk,akc->agc", table, returned, preferred_element_type=jnp.float32)
    atmosphere_next = (mixed_input.astype(jnp.float32) + jax.nn.gelu(response)).astype(jnp.bfloat16)
    forcing_coarse = jnp.einsum(
        "ogf,fc->ogc",
        flux_ocean.reshape(ocean_rows, half, flux_count),
        flux_embed.astype(jnp.float32),
        precision=highest,
    )
    forcing = jnp.broadcast_to(
        forcing_coarse[:, :, None, :], (ocean_rows, half, ratio, ocean_channels)
    ).reshape(ocean_rows, ocean_lon, ocean_channels)
    state = (ocean_state.astype(jnp.float32) + mask_value[:, :, None] * forcing).astype(
        jnp.bfloat16
    )
    windows = []
    for layer in range(layer_count):
        window = rims(state, radius)
        windows.append(window)
        update = cell_forward(
            depthwise(window, conv_kernel[layer]),
            norm_gain[layer],
            expand_weight[layer],
            project_weight[layer],
        )
        state = (state.astype(jnp.float32) + mask_value[:, :, None] * update).astype(jnp.bfloat16)
    cotangent = ocean_cotangent.astype(jnp.float32)
    for layer in range(layer_count - 1, -1, -1):
        hidden = depthwise(windows[layer], conv_kernel[layer])
        hidden_adjoint = cell_backward(
            hidden,
            norm_gain[layer],
            expand_weight[layer],
            project_weight[layer],
            mask_value,
            cotangent,
        )
        cotangent = cotangent + depthwise(
            rims(hidden_adjoint, radius), conv_kernel[layer, ::-1, ::-1]
        )
    forcing_adjoint = (
        (mask_value[:, :, None] * cotangent)
        .reshape(ocean_rows, half, ratio, ocean_channels)
        .sum(axis=2)
    )
    flux_ocean_adjoint = jnp.einsum(
        "ogc,fc->ogf", forcing_adjoint, flux_embed.astype(jnp.float32), precision=highest
    )
    flux_parts = jnp.dot(
        to_ocean.T, flux_ocean_adjoint.reshape(ocean_rows, half * flux_count), precision=highest
    )
    flux_adjoint = windows_to_rows(
        flux_parts.reshape(flux_parts.shape[0], half, flux_count), tiles
    )[None]
    from_flux = jnp.einsum(
        "agf,cf->agc", flux_adjoint, flux_read.astype(jnp.float32), precision=highest
    )
    atmosphere_adjoint = atmosphere_cotangent.astype(jnp.float32)
    _, gelu_back = jax.vjp(jax.nn.gelu, response)
    response_adjoint = gelu_back(atmosphere_adjoint)[0].astype(jnp.bfloat16)
    returned_adjoint = jnp.einsum(
        "gk,agc->akc", table, response_adjoint, preferred_element_type=jnp.float32
    ).astype(jnp.bfloat16)
    spectrum_adjoint = to_bands(
        spectral_adjoint(
            to_modes(returned_adjoint), legendre_forward, legendre_inverse, spectral_mix
        )
    )
    input_adjoint = atmosphere_adjoint + jnp.einsum(
        "gk,akc->agc", table, spectrum_adjoint, preferred_element_type=jnp.float32
    )
    atmosphere_grad = input_adjoint + from_flux
    surface_adjoint = jnp.einsum("agc,c->ag", input_adjoint, surface_embed, precision=highest)
    coarse_adjoint = jnp.dot(
        from_ocean, rows_to_windows(surface_adjoint[0], tiles), precision=highest
    )
    widened_adjoint = jnp.broadcast_to(
        coarse_adjoint[:, :, None], (ocean_rows, half, ratio)
    ).reshape(ocean_rows, ocean_lon)
    surface_grad = mask_value * widened_adjoint / ratio
    ocean_grad = (
        cotangent + surface_grad[:, :, None] * surface_read.astype(jnp.float32)[None, None, :]
    )
    return (atmosphere_next, state, atmosphere_grad, ocean_grad)


def solution(mesh):
    finer = Mesh(
        mesh.devices.reshape(mesh.shape["sec"], 4, 2, 4, 2),
        ("sec", "tile_0", "tile_1", "tile_2", "tile_3"),
    )
    placed = (
        P(SEC_TILE, None, None),
        P(TILE, "sec", None),
        P(TILE, "sec"),
        P(TILE, None),
        P(TILE, None, None, None),
        P(TILE, None, None, None),
        P(),
        P(),
        P(),
        P(),
        P(SEC_TILE, None, None),
        P(SEC_TILE, None, None),
        P(),
        P(),
        P(),
        P(),
        P(),
        P(SEC_TILE, None, None),
        P(TILE, "sec", None),
    )
    return jax.shard_map(
        per_device,
        mesh=finer,
        in_specs=placed,
        out_specs=(
            P(SEC_TILE, None, None),
            P(TILE, "sec", None),
            P(SEC_TILE, None, None),
            P(TILE, "sec", None),
        ),
        check_vma=False,
    )
```

```python
import functools
import jax
import jax.numpy as jnp
from jax import lax
from jax.experimental import pallas as pl
from jax.experimental.pallas import tpu as pltpu
from jax.sharding import Mesh
from jax.sharding import PartitionSpec as P

SEC_TILE = ("sec", "tile_0", "tile_1", "tile_2", "tile_3")
TILE = ("tile_0", "tile_1", "tile_2", "tile_3")
CHUNK = 80
PAD = 8
GELU_A = 0.7978845608028654
GELU_B = 0.044715


def fill_window(wide, own, above, below, west, east):
    radius = above.shape[0]
    rows, lon, _ = own.shape

    def put(source, first):
        def one(row, carry):
            wide[first + row, PAD : PAD + lon, :] = source[row].astype(jnp.float32)
            return carry

        lax.fori_loop(0, source.shape[0], one, 0)

    put(above, 0)
    put(own, radius)
    put(below, radius + rows)
    wide[:, 0:PAD, :] = west[...]
    wide[:, PAD + lon : PAD + lon + PAD, :] = east[...]


def convolve(wide, taps, out, start, rows, cols, side, group=2):
    radius = side // 2
    span = 8 * group

    def one(step, carry):
        left = start + step * span + PAD - radius
        total = [[None] * group for _ in range(rows)]
        for v in range(side):
            weight = [taps[u * side + v] for u in range(side)]
            for r in range(rows + 2 * radius):
                for k in range(group):
                    piece = wide[r, pl.ds(left + v + 8 * k, 8), :]
                    for u in range(side):
                        o = r - u
                        if 0 <= o < rows:
                            term = piece * weight[u]
                            total[o][k] = term if total[o][k] is None else total[o][k] + term
        for o in range(rows):
            for k in range(group):
                out[o, pl.ds(step * span + 8 * k, 8), :] = total[o][k]
        return carry

    lax.fori_loop(0, cols // span, one, 0)


def normalized(hidden):
    count = hidden.shape[-1]
    center = hidden - jnp.sum(hidden, axis=-1, keepdims=True) * (1.0 / count)
    inverse_std = lax.rsqrt(
        jnp.sum(center * center, axis=-1, keepdims=True) * (1.0 / count) + 1e-06
    )
    return center * inverse_std, inverse_std


def dot(a, b):
    return jnp.dot(a, b, preferred_element_type=jnp.float32)


def gelu_value(v):
    t = jnp.tanh(v * (GELU_A + (GELU_A * GELU_B) * (v * v)))
    h = 0.5 * v
    return h + h * t


def gelu_both(v):
    v2 = v * v
    t = jnp.tanh(v * (GELU_A + (GELU_A * GELU_B) * v2))
    h = 0.5 * v
    slope = (0.5 + 0.5 * t) + h * (1.0 - t * t) * (GELU_A + (3.0 * GELU_A * GELU_B) * v2)
    return h + h * t, slope


def backward_cell(unit, inverse_std, slope, masked, gain, expand_t, project_t):
    count = unit.shape[-1]
    before_adj = (slope * dot(masked, project_t)).astype(jnp.bfloat16)
    scaled = dot(before_adj, expand_t) * gain
    mean = jnp.sum(scaled, axis=-1, keepdims=True) * (1.0 / count)
    along = jnp.sum(scaled * unit, axis=-1, keepdims=True) * (1.0 / count)
    return (inverse_std * (scaled - mean - unit * along)).astype(jnp.bfloat16)


def flat(x):
    return x.reshape(x.shape[0] * x.shape[1], x.shape[2])


def forward_kernel(own, above, below, west, east, taps, gain, expand, project, mask, state, hidden, wide, *, side):
    step = pl.program_id(0)
    rows, cols, ch = state.shape

    @pl.when(step == 0)
    def _():
        fill_window(wide, own, above, below, west, east)

    start = pl.multiple_of(step * cols, cols)
    convolve(wide, taps, hidden, start, rows, cols, side)
    unit, _ = normalized(flat(hidden[...]))
    normed = (unit * gain[...]).astype(jnp.bfloat16)
    active = gelu_value(dot(normed, expand[...])).astype(jnp.bfloat16)
    update = dot(active, project[...])
    held = flat(own[:, pl.ds(start, cols), :]).astype(jnp.float32)
    new = held + flat(mask[...]).astype(jnp.float32) * update
    state[...] = new.astype(jnp.bfloat16).reshape(rows, cols, ch)


def turn_kernel(own, above, below, west, east, taps, gain, expand, project, expand_t, project_t, mask, cotangent, state, adjoint, wide, hidden, *, side):
    step = pl.program_id(0)
    rows, cols, ch = state.shape

    @pl.when(step == 0)
    def _():
        fill_window(wide, own, above, below, west, east)

    start = pl.multiple_of(step * cols, cols)
    convolve(wide, taps, hidden, start, rows, cols, side)
    unit, inverse_std = normalized(flat(hidden[...]))
    normed = (unit * gain[...]).astype(jnp.bfloat16)
    value, slope = gelu_both(dot(normed, expand[...]))
    update = dot(value.astype(jnp.bfloat16), project[...])
    weight = flat(mask[...])
    held = flat(own[:, pl.ds(start, cols), :]).astype(jnp.float32)
    new = held + weight.astype(jnp.float32) * update
    state[...] = new.astype(jnp.bfloat16).reshape(rows, cols, ch)
    masked = weight * flat(cotangent[...])
    result = backward_cell(unit, inverse_std, slope, masked, gain[...], expand_t[...], project_t[...])
    adjoint[...] = result.reshape(rows, cols, ch)


def backward_kernel(own, above, below, west, east, taps, gain, expand, expand_t, project_t, mask, cotangent, hidden, total, adjoint, wide, *, side):
    step = pl.program_id(0)
    rows, cols, ch = total.shape

    @pl.when(step == 0)
    def _():
        fill_window(wide, own, above, below, west, east)

    start = pl.multiple_of(step * cols, cols)
    convolve(wide, taps, total, start, rows, cols, side)
    summed = flat(cotangent[...]).astype(jnp.float32) + flat(total[...])
    total[...] = summed.reshape(rows, cols, ch)
    unit, inverse_std = normalized(flat(hidden[...]))
    normed = (unit * gain[...]).astype(jnp.bfloat16)
    _, slope = gelu_both(dot(normed, expand[...]))
    masked = (flat(mask[...]).astype(jnp.float32) * summed).astype(jnp.bfloat16)
    result = backward_cell(unit, inverse_std, slope, masked, gain[...], expand_t[...], project_t[...])
    adjoint[...] = result.reshape(rows, cols, ch)


def split_dot(a, b):
    high = b.astype(jnp.bfloat16)
    low = (b - high.astype(jnp.float32)).astype(jnp.bfloat16)
    return dot(a, high) + dot(a, low)


def last_kernel(own, above, below, west, east, taps, gather, embed_t, read, coarse, mask, cotangent, grad, flux, wide, total, *, side):
    step = pl.program_id(0)
    rows, cols, ch = grad.shape

    @pl.when(step == 0)
    def _():
        fill_window(wide, own, above, below, west, east)

    start = pl.multiple_of(step * cols, cols)
    convolve(wide, taps, total, start, rows, cols, side)
    weight = flat(mask[...]).astype(jnp.float32)
    summed = flat(total[...]) + flat(cotangent[...])
    grouped = split_dot(gather[...], weight * summed)
    high = grouped.astype(jnp.bfloat16)
    low = (grouped - high.astype(jnp.float32)).astype(jnp.bfloat16)
    flux[0] = dot(high, embed_t[...]) + dot(low, embed_t[...])
    spread = split_dot(gather[...].T, coarse[0] * read[...])
    grad[...] = (summed + weight * spread).reshape(rows, cols, ch)


def whole(x):
    return pl.BlockSpec(x.shape, lambda i, n=x.ndim: (0,) * n)


def chunked(rows, lon, ch, kind):
    return (
        jax.ShapeDtypeStruct((rows, lon, ch), kind),
        pl.BlockSpec((rows, CHUNK, ch), lambda i: (0, i, 0)),
    )


def stepped(steps, rows, ch, kind):
    return (
        jax.ShapeDtypeStruct((steps, rows, ch), kind),
        pl.BlockSpec((1, rows, ch), lambda i: (i, 0, 0)),
    )


def streamed_spec(x, steps):
    if x.shape[0] == steps:
        return pl.BlockSpec((1, *x.shape[1:]), lambda i: (i, 0, 0))
    return pl.BlockSpec((x.shape[0], CHUNK, x.shape[2]), lambda i: (0, i, 0))


def ocean_call(kernel, name, window, fixed, streamed, outs, side, flops, scratch=0):
    rows, lon, ch = window[0].shape
    radius = side // 2
    steps = lon // CHUNK
    return pl.pallas_call(
        functools.partial(kernel, side=side),
        name=name,
        grid=(steps,),
        in_specs=[whole(x) for x in (*window, *fixed)]
        + [streamed_spec(x, steps) for x in streamed],
        out_specs=[spec for _, spec in outs],
        out_shape=[shape for shape, _ in outs],
        scratch_shapes=[
            pltpu.VMEM((rows + 2 * radius, lon + 2 * PAD, ch), jnp.float32),
            *[pltpu.VMEM((rows, CHUNK, ch), jnp.float32)] * scratch,
        ],
        cost_estimate=pl.CostEstimate(
            flops=flops, bytes_accessed=16 * rows * lon * ch, transcendentals=0
        ),
    )(*window, *fixed, *streamed)


def in_blocks(x, dim, size):
    lengths = x.shape
    blocks = x.reshape(*lengths[:dim], size, lengths[dim] // size, *lengths[dim + 1 :])
    return jnp.moveaxis(blocks, dim, 0)


def laid_out(blocks, dim):
    lengths = list(blocks.shape[1:])
    lengths[dim] *= blocks.shape[0]
    return jnp.moveaxis(blocks, 0, dim).reshape(lengths)


def turned_blocks(blocks, axes, sequence):
    lengths = [lax.axis_size(a) for a in axes]
    blocks = blocks.reshape(*lengths, *blocks.shape[1:])
    for k in sequence:
        blocks = lax.all_to_all(blocks, axes[k], split_axis=k, concat_axis=k, tiled=True)
    return blocks.reshape(-1, *blocks.shape[len(axes) :])


def two_step_exchange(x, groups, sequence, split_dim, concat_dim):
    size = lax.axis_size(groups[0]) * lax.axis_size(groups[1])
    blocks = in_blocks(x, split_dim, size)
    return laid_out(turned_blocks(blocks, groups, sequence), concat_dim)


def wave_table(lon_count, mode_count):
    longitude = jnp.arange(lon_count, dtype=jnp.int32)
    wavenumber = jnp.arange(mode_count, dtype=jnp.int32)
    phase = (longitude[:, None] * wavenumber[None, :] % lon_count).astype(jnp.float32) * (
        2.0 * jnp.pi / lon_count
    )
    scaled = jnp.stack([jnp.cos(phase), -jnp.sin(phase)], axis=2) * jnp.sqrt(
        jnp.float32(2.0 / lon_count)
    )
    return scaled.reshape(lon_count, 2 * mode_count).astype(jnp.bfloat16)


def mix_complex(coefficient, mix_real, mix_imag):
    real_part = coefficient[:, :, 0]
    imag_part = coefficient[:, :, 1]
    out_real = jnp.einsum(
        "lmc,cd->lmd", real_part, mix_real, preferred_element_type=jnp.float32
    ) - jnp.einsum("lmc,cd->lmd", imag_part, mix_imag, preferred_element_type=jnp.float32)
    out_imag = jnp.einsum(
        "lmc,cd->lmd", imag_part, mix_real, preferred_element_type=jnp.float32
    ) + jnp.einsum("lmc,cd->lmd", real_part, mix_imag, preferred_element_type=jnp.float32)
    return jnp.stack([out_real, out_imag], axis=2).astype(jnp.bfloat16)


def spectral_block(spectrum, forward, inverse, mixing):
    lat_count, columns, channels = spectrum.shape
    split = spectrum.reshape(lat_count, columns // 2, 2, channels)
    coefficient = jnp.einsum(
        "mla,amrc->lmrc", forward, split, preferred_element_type=jnp.float32
    ).astype(jnp.bfloat16)
    mixed = mix_complex(coefficient, mixing[0], mixing[1])
    returned = jnp.einsum(
        "mal,lmrc->amrc", inverse, mixed, preferred_element_type=jnp.float32
    ).astype(jnp.bfloat16)
    return returned.reshape(lat_count, columns, channels)


def spectral_adjoint(returned_adjoint, forward, inverse, mixing):
    lat_count, columns, channels = returned_adjoint.shape
    split = returned_adjoint.reshape(lat_count, columns // 2, 2, channels)
    mixed_adjoint = jnp.einsum(
        "mal,amrc->lmrc", inverse, split, preferred_element_type=jnp.float32
    ).astype(jnp.bfloat16)
    real_part = mixed_adjoint[:, :, 0]
    imag_part = mixed_adjoint[:, :, 1]
    back_real = jnp.einsum(
        "lmd,cd->lmc", real_part, mixing[0], preferred_element_type=jnp.float32
    ) + jnp.einsum("lmd,cd->lmc", imag_part, mixing[1], preferred_element_type=jnp.float32)
    back_imag = jnp.einsum(
        "lmd,cd->lmc", imag_part, mixing[0], preferred_element_type=jnp.float32
    ) - jnp.einsum("lmd,cd->lmc", real_part, mixing[1], preferred_element_type=jnp.float32)
    coefficient_adjoint = jnp.stack([back_real, back_imag], axis=2).astype(jnp.bfloat16)
    spectrum_adjoint = jnp.einsum(
        "mla,lmrc->amrc", forward, coefficient_adjoint, preferred_element_type=jnp.float32
    ).astype(jnp.bfloat16)
    return spectrum_adjoint.reshape(lat_count, columns, channels)


def to_modes(values):
    return two_step_exchange(
        values, (("sec", "tile_0", "tile_1", "tile_2"), "tile_3"), (1, 0), 1, 0
    )


def to_bands(values):
    return lax.all_to_all(values, SEC_TILE, split_axis=0, concat_axis=1, tiled=True)


def half_routes(tiles):
    bands = 2 * tiles
    straight = [(a, (a % 2) * tiles + a // 2) for a in range(bands)]
    crossed = [(a, (1 - a % 2) * tiles + a // 2) for a in range(bands)]
    return straight, crossed


def back(pairs):
    return [(j, i) for i, j in pairs]


def shift_tiles(values, step, tiles):
    pairs = [
        (s * tiles + j, s * tiles + j + step)
        for s in range(2)
        for j in range(tiles)
        if 0 <= j + step < tiles
    ]
    return lax.ppermute(values, SEC_TILE, pairs)


def rim_pieces(values, width, tiles):
    above = shift_tiles(values[-width:], 1, tiles)
    below = shift_tiles(values[:width], -1, tiles)
    sides = jnp.concatenate([values[:, :width], values[:, -width:]], axis=1)
    other = lax.ppermute(sides, "sec", [(0, 1), (1, 0)])

    def across(part, step):
        pairs = [
            (s * tiles + j, (1 - s) * tiles + j + step)
            for s in range(2)
            for j in range(tiles)
            if 0 <= j + step < tiles
        ]
        return lax.ppermute(part, SEC_TILE, pairs)

    columns = jnp.concatenate(
        [across(sides[-width:], 1), other, across(sides[:width], -1)], axis=0
    ).astype(jnp.float32)
    spare = PAD - width
    west = jnp.pad(columns[:, width:], ((0, 0), (spare, 0), (0, 0)))
    east = jnp.pad(columns[:, :width], ((0, 0), (0, spare), (0, 0)))
    return values, above, below, west, east


def broad_taps(kernel):
    side, _, ch = kernel.shape
    return jnp.broadcast_to(
        kernel.astype(jnp.float32).reshape(side * side, 1, ch), (side * side, 8, ch)
    )


def window_matrix(bands_row, blocks, tiles):
    base = 2 * lax.axis_index(TILE) - 2
    onehot = (
        (bands_row - base)[:, None] == jnp.arange(8, dtype=jnp.int32)[None, :]
    ).astype(jnp.float32)
    return jnp.sum(blocks[:, :, None] * onehot[:, None, :], axis=0)


def rows_to_windows(values, tiles):
    lon = values.shape[0]
    halves = values.reshape(2, lon // 2, *values.shape[1:])
    odd = lax.axis_index(SEC_TILE) % 2 == 1
    straight, crossed = half_routes(tiles)
    first = lax.ppermute(jnp.where(odd, halves[1], halves[0]), SEC_TILE, straight)
    second = lax.ppermute(jnp.where(odd, halves[0], halves[1]), SEC_TILE, crossed)
    east = lax.axis_index("sec") == 1
    pair = jnp.stack([jnp.where(east, second, first), jnp.where(east, first, second)])
    parts = [
        shift_tiles(pair, 1, tiles),
        pair,
        shift_tiles(pair, -1, tiles),
        shift_tiles(pair, -2, tiles),
    ]
    return jnp.concatenate(parts, axis=0)


def windows_to_rows(parts, tiles):
    pair = (
        parts[2:4]
        + shift_tiles(parts[0:2], -1, tiles)
        + shift_tiles(parts[4:6], 1, tiles)
        + shift_tiles(parts[6:8], 2, tiles)
    )
    east = lax.axis_index("sec") == 1
    straight, crossed = half_routes(tiles)
    first = lax.ppermute(jnp.where(east, pair[1], pair[0]), SEC_TILE, back(straight))
    second = lax.ppermute(jnp.where(east, pair[0], pair[1]), SEC_TILE, back(crossed))
    odd = lax.axis_index(SEC_TILE) % 2 == 1
    return jnp.concatenate([jnp.where(odd, second, first), jnp.where(odd, first, second)])


def per_device(
    atmosphere,
    ocean_state,
    land_mask,
    crossing_bands,
    ocean_regrid,
    atmosphere_regrid,
    surface_read,
    surface_embed,
    flux_read,
    flux_embed,
    legendre_forward,
    legendre_inverse,
    spectral_mix,
    conv_kernel,
    norm_gain,
    expand_weight,
    project_weight,
    atmosphere_cotangent,
    ocean_cotangent,
):
    band_total = lax.axis_size(SEC_TILE)
    lat_rows, lon_count, channels = atmosphere.shape
    lat_count = lat_rows * band_total
    ocean_rows, ocean_lon, ocean_channels = ocean_state.shape
    half = lon_count // lax.axis_size("sec")
    ratio = ocean_lon // half
    flux_count = flux_read.shape[1]
    radius = conv_kernel.shape[1] // 2
    highest = lax.Precision.HIGHEST
    mask_value = land_mask.astype(jnp.float32)
    tiles = lax.axis_size(TILE)
    to_ocean = window_matrix(crossing_bands[0], ocean_regrid[0, :, :, 0], tiles)
    from_ocean = window_matrix(crossing_bands[0], atmosphere_regrid[0, :, 0, :], tiles)
    surface = jnp.dot(ocean_state, surface_read, preferred_element_type=jnp.float32)
    coarse = jnp.mean((mask_value * surface).reshape(ocean_rows, half, ratio), axis=2)
    surface_atmosphere = windows_to_rows(
        jnp.sum(from_ocean[:, :, None] * coarse[:, None, :], axis=0), tiles
    )[None]
    flux = jnp.einsum("agc,cf->agf", atmosphere, flux_read, preferred_element_type=jnp.float32)
    flux_window = rows_to_windows(flux[0], tiles)
    flux_ocean = jnp.dot(
        to_ocean, flux_window.reshape(flux_window.shape[0], half * flux_count), precision=highest
    )
    mixed_input = (
        atmosphere.astype(jnp.float32)
        + surface_atmosphere[:, :, None] * surface_embed[None, None, :]
    ).astype(jnp.bfloat16)
    table = wave_table(lon_count, legendre_forward.shape[0] * band_total)
    spectrum = jnp.einsum(
        "gk,agc->akc", table, mixed_input, preferred_element_type=jnp.float32
    ).astype(jnp.bfloat16)
    returned = to_bands(
        spectral_block(to_modes(spectrum), legendre_forward, legendre_inverse, spectral_mix)
    )
    response = jnp.einsum("gk,akc->agc", table, returned, preferred_element_type=jnp.float32)
    atmosphere_next = (mixed_input.astype(jnp.float32) + jax.nn.gelu(response)).astype(jnp.bfloat16)
    forcing_coarse = jnp.einsum(
        "ogf,fc->ogc",
        flux_ocean.reshape(ocean_rows, half, flux_count),
        flux_embed.astype(jnp.float32),
        precision=highest,
    )
    forcing = jnp.broadcast_to(
        forcing_coarse[:, :, None, :], (ocean_rows, half, ratio, ocean_channels)
    ).reshape(ocean_rows, ocean_lon, ocean_channels)
    state = (ocean_state.astype(jnp.float32) + mask_value[:, :, None] * forcing).astype(
        jnp.bfloat16
    )
    side = conv_kernel.shape[1]
    wet = jnp.broadcast_to(land_mask[:, :, None], ocean_state.shape).astype(jnp.bfloat16)
    gains = norm_gain[:, None, :]
    expand_t = jnp.swapaxes(expand_weight, 1, 2)
    project_t = jnp.swapaxes(project_weight, 1, 2)
    cells = ocean_rows * ocean_lon
    work = 2 * cells * ocean_channels * side * side
    product = 2 * cells * ocean_channels * expand_weight.shape[2]
    state_1, hidden_0 = ocean_call(
        forward_kernel,
        "first_block",
        rim_pieces(state, radius, tiles),
        (broad_taps(conv_kernel[0]), gains[0], expand_weight[0], project_weight[0]),
        (wet,),
        [chunked(ocean_rows, ocean_lon, ocean_channels, t) for t in (jnp.bfloat16, jnp.float32)],
        side,
        work + 2 * product,
    )
    state_2, adjoint_1 = ocean_call(
        turn_kernel,
        "second_block",
        rim_pieces(state_1, radius, tiles),
        (
            broad_taps(conv_kernel[1]),
            gains[1],
            expand_weight[1],
            project_weight[1],
            expand_t[1],
            project_t[1],
        ),
        (wet, ocean_cotangent),
        [chunked(ocean_rows, ocean_lon, ocean_channels, jnp.bfloat16)] * 2,
        side,
        work + 4 * product,
        1,
    )
    cotangent_1, adjoint_0 = ocean_call(
        backward_kernel,
        "first_block_back",
        rim_pieces(adjoint_1, radius, tiles),
        (
            broad_taps(conv_kernel[1, ::-1, ::-1]),
            gains[0],
            expand_weight[0],
            expand_t[0],
            project_t[0],
        ),
        (wet, ocean_cotangent, hidden_0),
        [chunked(ocean_rows, ocean_lon, ocean_channels, t) for t in (jnp.float32, jnp.bfloat16)],
        side,
        work + 3 * product,
    )
    atmosphere_adjoint = atmosphere_cotangent.astype(jnp.float32)
    _, gelu_back = jax.vjp(jax.nn.gelu, response)
    response_adjoint = gelu_back(atmosphere_adjoint)[0].astype(jnp.bfloat16)
    returned_adjoint = jnp.einsum(
        "gk,agc->akc", table, response_adjoint, preferred_element_type=jnp.float32
    ).astype(jnp.bfloat16)
    spectrum_adjoint = to_bands(
        spectral_adjoint(
            to_modes(returned_adjoint), legendre_forward, legendre_inverse, spectral_mix
        )
    )
    input_adjoint = atmosphere_adjoint + jnp.einsum(
        "gk,akc->agc", table, spectrum_adjoint, preferred_element_type=jnp.float32
    )
    surface_adjoint = jnp.einsum("agc,c->ag", input_adjoint, surface_embed, precision=highest)
    coarse_adjoint = jnp.dot(
        from_ocean, rows_to_windows(surface_adjoint[0], tiles), precision=highest
    )
    steps = ocean_lon // CHUNK
    coarse_chunk = CHUNK // ratio
    coarse_blocks = (
        jnp.swapaxes((coarse_adjoint / ratio).reshape(ocean_rows, steps, coarse_chunk), 0, 1)
    ).reshape(steps, ocean_rows * coarse_chunk, 1)
    gather = (
        jnp.arange(ocean_rows * coarse_chunk, dtype=jnp.int32)[:, None]
        == jnp.arange(ocean_rows * CHUNK, dtype=jnp.int32)[None, :] // ratio
    ).astype(jnp.bfloat16)
    ocean_grad, flux_blocks = ocean_call(
        last_kernel,
        "ocean_gradient",
        rim_pieces(adjoint_0, radius, tiles),
        (
            broad_taps(conv_kernel[0, ::-1, ::-1]),
            gather,
            flux_embed.T,
            surface_read.astype(jnp.float32)[None, :],
        ),
        (coarse_blocks, wet, cotangent_1),
        [
            chunked(ocean_rows, ocean_lon, ocean_channels, jnp.float32),
            stepped(steps, ocean_rows * coarse_chunk, flux_count, jnp.float32),
        ],
        side,
        work,
        1,
    )
    flux_ocean_adjoint = jnp.swapaxes(
        flux_blocks.reshape(steps, ocean_rows, coarse_chunk, flux_count), 0, 1
    ).reshape(ocean_rows, half, flux_count)
    flux_parts = jnp.dot(
        to_ocean.T, flux_ocean_adjoint.reshape(ocean_rows, half * flux_count), precision=highest
    )
    flux_adjoint = windows_to_rows(
        flux_parts.reshape(flux_parts.shape[0], half, flux_count), tiles
    )[None]
    from_flux = jnp.einsum(
        "agf,cf->agc", flux_adjoint, flux_read.astype(jnp.float32), precision=highest
    )
    atmosphere_grad = input_adjoint + from_flux
    return (atmosphere_next, state_2, atmosphere_grad, ocean_grad)


def solution(mesh):
    finer = Mesh(
        mesh.devices.reshape(mesh.shape["sec"], 4, 2, 4, 2),
        ("sec", "tile_0", "tile_1", "tile_2", "tile_3"),
    )
    placed = (
        P(SEC_TILE, None, None),
        P(TILE, "sec", None),
        P(TILE, "sec"),
        P(TILE, None),
        P(TILE, None, None, None),
        P(TILE, None, None, None),
        P(),
        P(),
        P(),
        P(),
        P(SEC_TILE, None, None),
        P(SEC_TILE, None, None),
        P(),
        P(),
        P(),
        P(),
        P(),
        P(SEC_TILE, None, None),
        P(TILE, "sec", None),
    )
    return jax.shard_map(
        per_device,
        mesh=finer,
        in_specs=placed,
        out_specs=(
            P(SEC_TILE, None, None),
            P(TILE, "sec", None),
            P(SEC_TILE, None, None),
            P(TILE, "sec", None),
        ),
        check_vma=False,
    )
```

```python
import functools
import jax
import jax.numpy as jnp
from jax import lax
from jax.experimental import pallas as pl
from jax.experimental.pallas import tpu as pltpu
from jax.sharding import Mesh
from jax.sharding import PartitionSpec as P

SEC_TILE = ("sec", "tile_0", "tile_1", "tile_2", "tile_3")
TILE = ("tile_0", "tile_1", "tile_2", "tile_3")
CHUNK = 80
PAD = 8
GELU_A = 0.7978845608028654
GELU_B = 0.044715


def fill_window(wide, place, own, near, far, other, near_corner, far_corner):
    radius = near.shape[0]
    _, lon, _ = own.shape
    inside = place[2].astype(jnp.float32)

    def put(source, sides, first, scale):
        def one(row, carry):
            value = source[row].astype(jnp.float32)
            edges = sides[row].astype(jnp.float32)
            if scale is not None:
                value = value * scale
                edges = edges * scale
            wide[first + row, PAD : PAD + lon, :] = value
            wide[first + row, 0:PAD, :] = edges[0:PAD]
            wide[first + row, PAD + lon : PAD + lon + PAD, :] = edges[PAD : 2 * PAD]
            return carry

        lax.fori_loop(0, source.shape[0], one, 0)

    put(near, near_corner, place[0], None)
    put(own, other, radius, None)
    put(far, far_corner, place[1], inside)


def fill_taps(broad, taps, flipped):
    count = taps.shape[0]
    for k in range(count):
        row = count - 1 - k if flipped else k
        broad[k] = jnp.broadcast_to(taps[row : row + 1, :], broad.shape[1:])


def put_rims(near_out, far_out, place, value):
    rows, radius = value.shape[0], near_out.shape[0]
    top, bottom = value[:radius], value[rows - radius :]
    first = place[3] == 0
    near_out[...] = jnp.where(first, bottom, top)
    far_out[...] = jnp.where(first, top, bottom)


def convolve(wide, broad, out, start, rows, cols, side, group=2):
    radius = side // 2
    span = 8 * group

    def one(step, carry):
        left = start + step * span + PAD - radius
        total = [[None] * group for _ in range(rows)]
        for v in range(side):
            weight = [broad[u * side + v] for u in range(side)]
            for r in range(rows + 2 * radius):
                for k in range(group):
                    piece = wide[r, pl.ds(left + v + 8 * k, 8), :]
                    for u in range(side):
                        o = r - u
                        if 0 <= o < rows:
                            term = piece * weight[u]
                            total[o][k] = term if total[o][k] is None else total[o][k] + term
        for o in range(rows):
            for k in range(group):
                out[o, pl.ds(step * span + 8 * k, 8), :] = total[o][k]
        return carry

    lax.fori_loop(0, cols // span, one, 0)


def normalized(hidden):
    count = hidden.shape[-1]
    center = hidden - jnp.sum(hidden, axis=-1, keepdims=True) * (1.0 / count)
    inverse_std = lax.rsqrt(
        jnp.sum(center * center, axis=-1, keepdims=True) * (1.0 / count) + 1e-06
    )
    return center * inverse_std, inverse_std


def dot(a, b):
    return jnp.dot(a, b, preferred_element_type=jnp.float32)


def gelu_value(v):
    t = jnp.tanh(v * (GELU_A + (GELU_A * GELU_B) * (v * v)))
    h = 0.5 * v
    return h + h * t


def gelu_both(v):
    v2 = v * v
    t = jnp.tanh(v * (GELU_A + (GELU_A * GELU_B) * v2))
    h = 0.5 * v
    slope = (0.5 + 0.5 * t) + h * (1.0 - t * t) * (GELU_A + (3.0 * GELU_A * GELU_B) * v2)
    return h + h * t, slope


def backward_cell(unit, inverse_std, slope, masked, gain, expand_t, project_t):
    count = unit.shape[-1]
    before_adj = (slope * dot(masked, project_t)).astype(jnp.bfloat16)
    scaled = dot(before_adj, expand_t) * gain
    mean = jnp.sum(scaled, axis=-1, keepdims=True) * (1.0 / count)
    along = jnp.sum(scaled * unit, axis=-1, keepdims=True) * (1.0 / count)
    return (inverse_std * (scaled - mean - unit * along)).astype(jnp.bfloat16)


def flat(x):
    return x.reshape(x.shape[0] * x.shape[1], x.shape[2])


def forward_kernel(place, own, near, far, other, near_corner, far_corner, taps, gain, expand, project, mask, state, near_out, far_out, hidden, wide, broad, *, side):
    step = pl.program_id(0)
    rows, cols, ch = state.shape

    @pl.when(step == 0)
    def _():
        fill_window(wide, place, own, near, far, other, near_corner, far_corner)
        fill_taps(broad, taps, False)

    start = pl.multiple_of(step * cols, cols)
    convolve(wide, broad, hidden, start, rows, cols, side)
    unit, _ = normalized(flat(hidden[...]))
    normed = (unit * gain[...]).astype(jnp.bfloat16)
    active = gelu_value(dot(normed, expand[...])).astype(jnp.bfloat16)
    update = dot(active, project[...])
    held = flat(own[:, pl.ds(start, cols), :]).astype(jnp.float32)
    new = held + flat(mask[...]).astype(jnp.float32) * update
    result = new.astype(jnp.bfloat16).reshape(rows, cols, ch)
    state[...] = result
    put_rims(near_out, far_out, place, result)


def turn_kernel(place, own, near, far, other, near_corner, far_corner, taps, gain, expand, project, expand_t, project_t, mask, cotangent, state, adjoint, near_out, far_out, wide, broad, hidden, *, side):
    step = pl.program_id(0)
    rows, cols, ch = state.shape

    @pl.when(step == 0)
    def _():
        fill_window(wide, place, own, near, far, other, near_corner, far_corner)
        fill_taps(broad, taps, False)

    start = pl.multiple_of(step * cols, cols)
    convolve(wide, broad, hidden, start, rows, cols, side)
    unit, inverse_std = normalized(flat(hidden[...]))
    normed = (unit * gain[...]).astype(jnp.bfloat16)
    value, slope = gelu_both(dot(normed, expand[...]))
    update = dot(value.astype(jnp.bfloat16), project[...])
    weight = flat(mask[...])
    held = flat(own[:, pl.ds(start, cols), :]).astype(jnp.float32)
    new = held + weight.astype(jnp.float32) * update
    state[...] = new.astype(jnp.bfloat16).reshape(rows, cols, ch)
    masked = weight * flat(cotangent[...])
    result = backward_cell(unit, inverse_std, slope, masked, gain[...], expand_t[...], project_t[...])
    result = result.reshape(rows, cols, ch)
    adjoint[...] = result
    put_rims(near_out, far_out, place, result)


def backward_kernel(place, own, near, far, other, near_corner, far_corner, taps, gain, expand, expand_t, project_t, mask, cotangent, hidden, total, adjoint, near_out, far_out, wide, broad, *, side):
    step = pl.program_id(0)
    rows, cols, ch = total.shape

    @pl.when(step == 0)
    def _():
        fill_window(wide, place, own, near, far, other, near_corner, far_corner)
        fill_taps(broad, taps, True)

    start = pl.multiple_of(step * cols, cols)
    convolve(wide, broad, total, start, rows, cols, side)
    summed = flat(cotangent[...]).astype(jnp.float32) + flat(total[...])
    total[...] = summed.reshape(rows, cols, ch)
    unit, inverse_std = normalized(flat(hidden[...]))
    normed = (unit * gain[...]).astype(jnp.bfloat16)
    _, slope = gelu_both(dot(normed, expand[...]))
    masked = (flat(mask[...]).astype(jnp.float32) * summed).astype(jnp.bfloat16)
    result = backward_cell(unit, inverse_std, slope, masked, gain[...], expand_t[...], project_t[...])
    result = result.reshape(rows, cols, ch)
    adjoint[...] = result
    put_rims(near_out, far_out, place, result)


def split_dot(a, b):
    high = b.astype(jnp.bfloat16)
    low = (b - high.astype(jnp.float32)).astype(jnp.bfloat16)
    return dot(a, high) + dot(a, low)


def last_kernel(place, own, near, far, other, near_corner, far_corner, taps, gather, embed_t, mask, cotangent, total, flux, wide, broad, *, side):
    step = pl.program_id(0)
    rows, cols, ch = total.shape

    @pl.when(step == 0)
    def _():
        fill_window(wide, place, own, near, far, other, near_corner, far_corner)
        fill_taps(broad, taps, True)

    start = pl.multiple_of(step * cols, cols)
    convolve(wide, broad, total, start, rows, cols, side)
    summed = flat(total[...]) + flat(cotangent[...])
    total[...] = summed.reshape(rows, cols, ch)
    grouped = split_dot(gather[...], flat(mask[...]).astype(jnp.float32) * summed)
    high = grouped.astype(jnp.bfloat16)
    low = (grouped - high.astype(jnp.float32)).astype(jnp.bfloat16)
    flux[0] = dot(high, embed_t[...]) + dot(low, embed_t[...])


def surface_kernel(spread, read, coarse, mask, cotangent, grad):
    rows, cols, ch = grad.shape
    added = split_dot(spread[...], coarse[0] * read[...])
    weight = flat(mask[...]).astype(jnp.float32)
    grad[...] = (flat(cotangent[...]) + weight * added).reshape(rows, cols, ch)


def surface_call(spread, read, coarse, mask, cotangent):
    rows, lon, ch = cotangent.shape
    steps = lon // CHUNK
    shape, spec = chunked(rows, lon, ch, jnp.float32)
    return pl.pallas_call(
        surface_kernel,
        name="surface_gradient",
        grid=(steps,),
        in_specs=[whole(spread), whole(read)]
        + [streamed_spec(x, steps) for x in (coarse, mask, cotangent)],
        out_specs=spec,
        out_shape=shape,
        cost_estimate=pl.CostEstimate(
            flops=4 * rows * lon * ch, bytes_accessed=10 * rows * lon * ch, transcendentals=0
        ),
    )(spread, read, coarse, mask, cotangent)


def whole(x):
    return pl.BlockSpec(x.shape, lambda i, n=x.ndim: (0,) * n)


def chunked(rows, lon, ch, kind):
    return (
        jax.ShapeDtypeStruct((rows, lon, ch), kind),
        pl.BlockSpec((rows, CHUNK, ch), lambda i: (0, i, 0)),
    )


def stepped(steps, rows, ch, kind):
    return (
        jax.ShapeDtypeStruct((steps, rows, ch), kind),
        pl.BlockSpec((1, rows, ch), lambda i: (i, 0, 0)),
    )


def streamed_spec(x, steps):
    if x.shape[0] == steps:
        return pl.BlockSpec((1, *x.shape[1:]), lambda i: (i, 0, 0))
    return pl.BlockSpec((x.shape[0], CHUNK, x.shape[2]), lambda i: (0, i, 0))


def ocean_call(kernel, window, fixed, streamed, outs, side, flops, scratch=0):
    rows, lon, ch = window[1].shape
    radius = side // 2
    steps = lon // CHUNK
    return pl.pallas_call(
        functools.partial(kernel, side=side),
        grid=(steps,),
        in_specs=[pl.BlockSpec(memory_space=pltpu.SMEM)]
        + [whole(x) for x in (*window[1:], *fixed)]
        + [streamed_spec(x, steps) for x in streamed],
        out_specs=[spec for _, spec in outs],
        out_shape=[shape for shape, _ in outs],
        scratch_shapes=[
            pltpu.VMEM((rows + 2 * radius, lon + 2 * PAD, ch), jnp.float32),
            pltpu.VMEM((side * side, 8, ch), jnp.float32),
            *[pltpu.VMEM((rows, CHUNK, ch), jnp.float32)] * scratch,
        ],
        cost_estimate=pl.CostEstimate(
            flops=flops, bytes_accessed=16 * rows * lon * ch, transcendentals=0
        ),
    )(*window, *fixed, *streamed)


def wave_table(lon_count, mode_count):
    longitude = jnp.arange(lon_count, dtype=jnp.int32)
    wavenumber = jnp.arange(mode_count, dtype=jnp.int32)
    phase = (longitude[:, None] * wavenumber[None, :] % lon_count).astype(jnp.float32) * (
        2.0 * jnp.pi / lon_count
    )
    scaled = jnp.stack([jnp.cos(phase), -jnp.sin(phase)], axis=2) * jnp.sqrt(
        jnp.float32(2.0 / lon_count)
    )
    return scaled.reshape(lon_count, 2 * mode_count).astype(jnp.bfloat16)


def mix_complex(coefficient, mix_real, mix_imag):
    real_part = coefficient[:, :, 0]
    imag_part = coefficient[:, :, 1]
    out_real = jnp.einsum(
        "lmc,cd->lmd", real_part, mix_real, preferred_element_type=jnp.float32
    ) - jnp.einsum("lmc,cd->lmd", imag_part, mix_imag, preferred_element_type=jnp.float32)
    out_imag = jnp.einsum(
        "lmc,cd->lmd", imag_part, mix_real, preferred_element_type=jnp.float32
    ) + jnp.einsum("lmc,cd->lmd", real_part, mix_imag, preferred_element_type=jnp.float32)
    return jnp.stack([out_real, out_imag], axis=2).astype(jnp.bfloat16)


def spectral_block(spectrum, forward, inverse, mixing):
    lat_count, columns, channels = spectrum.shape
    split = spectrum.reshape(lat_count, columns // 2, 2, channels)
    coefficient = jnp.einsum(
        "mla,amrc->lmrc", forward, split, preferred_element_type=jnp.float32
    ).astype(jnp.bfloat16)
    mixed = mix_complex(coefficient, mixing[0], mixing[1])
    returned = jnp.einsum(
        "mal,lmrc->amrc", inverse, mixed, preferred_element_type=jnp.float32
    ).astype(jnp.bfloat16)
    return returned.reshape(lat_count, columns, channels)


def spectral_adjoint(returned_adjoint, forward, inverse, mixing):
    lat_count, columns, channels = returned_adjoint.shape
    split = returned_adjoint.reshape(lat_count, columns // 2, 2, channels)
    mixed_adjoint = jnp.einsum(
        "mal,amrc->lmrc", inverse, split, preferred_element_type=jnp.float32
    ).astype(jnp.bfloat16)
    real_part = mixed_adjoint[:, :, 0]
    imag_part = mixed_adjoint[:, :, 1]
    back_real = jnp.einsum(
        "lmd,cd->lmc", real_part, mixing[0], preferred_element_type=jnp.float32
    ) + jnp.einsum("lmd,cd->lmc", imag_part, mixing[1], preferred_element_type=jnp.float32)
    back_imag = jnp.einsum(
        "lmd,cd->lmc", imag_part, mixing[0], preferred_element_type=jnp.float32
    ) - jnp.einsum("lmd,cd->lmc", real_part, mixing[1], preferred_element_type=jnp.float32)
    coefficient_adjoint = jnp.stack([back_real, back_imag], axis=2).astype(jnp.bfloat16)
    spectrum_adjoint = jnp.einsum(
        "mla,lmrc->amrc", forward, coefficient_adjoint, preferred_element_type=jnp.float32
    ).astype(jnp.bfloat16)
    return spectrum_adjoint.reshape(lat_count, columns, channels)


UPPER = ("sec", "tile_0", "tile_1", "tile_2")


def swap_core(values):
    return lax.ppermute(values, "tile_3", [(0, 1), (1, 0)])


def core_turn(parts):
    first = lax.axis_index("tile_3") == 0
    kept = jnp.where(first, parts[:, 0], parts[:, 1])
    got = swap_core(jnp.where(first, parts[:, 1], parts[:, 0]))
    return jnp.stack([jnp.where(first, kept, got), jnp.where(first, got, kept)], axis=1)


def to_modes(values):
    _, columns, ch = values.shape
    upper = lax.axis_size(UPPER)
    parts = core_turn(values.reshape(upper, 2, columns // (2 * upper), ch))
    parts = lax.all_to_all(parts, UPPER, split_axis=0, concat_axis=0, tiled=True)
    return parts.reshape(2 * upper, columns // (2 * upper), ch)


def to_bands(values):
    bands, columns, ch = values.shape
    upper = lax.axis_size(UPPER)
    parts = values.reshape(upper, 2, columns, ch)
    parts = lax.all_to_all(parts, UPPER, split_axis=0, concat_axis=0, tiled=True)
    return core_turn(parts).reshape(1, bands * columns, ch)


def half_routes(tiles):
    bands = 2 * tiles
    straight = [(a, (a % 2) * tiles + a // 2) for a in range(bands)]
    crossed = [(a, (1 - a % 2) * tiles + a // 2) for a in range(bands)]
    return straight, crossed


def back(pairs):
    return [(j, i) for i, j in pairs]


def shift_tiles(values, step, tiles):
    pairs = [
        (s * tiles + j, s * tiles + (j + step) % tiles)
        for s in range(2)
        for j in range(tiles)
    ]
    return lax.ppermute(values, SEC_TILE, pairs)


def near_swap(values, cross, tiles):
    pairs = [
        (s * tiles + j, (s ^ cross) * tiles + (j ^ 1)) for s in range(2) for j in range(tiles)
    ]
    return lax.ppermute(values, SEC_TILE, pairs)


def far_swap(values, cross, tiles):
    def partner(j):
        return j if j in (0, tiles - 1) else j + (1 if j % 2 == 1 else -1)

    pairs = [
        (s * tiles + j, (s ^ cross) * tiles + partner(j)) for s in range(2) for j in range(tiles)
    ]
    return lax.ppermute(values, SEC_TILE, pairs)


def send_rows(values, width, near):
    rows = values.shape[0]
    first = lax.axis_index("tile_3") == 0
    start = jnp.where(first, rows - width, 0) if near else jnp.where(first, 0, rows - width)
    return lax.dynamic_slice_in_dim(values, start, width, 0)


def rim_pieces(values, near_rows, far_rows, width, tiles):
    near = near_swap(near_rows, 0, tiles)
    far = far_swap(far_rows, 0, tiles)
    spare = ((0, 0), (0, PAD - width), (0, 0))
    sides = jnp.concatenate(
        [
            jnp.pad(values[:, -width:], (spare[0], spare[1][::-1], spare[2])),
            jnp.pad(values[:, :width], spare),
        ],
        axis=1,
    )
    other = lax.ppermute(sides, "sec", [(0, 1), (1, 0)])
    near_corner = near_swap(send_rows(sides, width, True), 1, tiles)
    far_corner = far_swap(send_rows(sides, width, False), 1, tiles)
    core = lax.axis_index("tile_3")
    tile = lax.axis_index(TILE)
    rows = values.shape[0]
    place = jnp.stack(
        [
            jnp.where(core == 0, rows + width, 0),
            jnp.where(core == 0, 0, rows + width),
            jnp.where((tile == 0) | (tile == tiles - 1), 0, 1),
            core,
        ]
    ).astype(jnp.int32)
    return place, values, near, far, other, near_corner, far_corner


def window_matrix(bands_row, blocks):
    base = 2 * lax.axis_index(TILE) - 2
    onehot = (
        (bands_row - base)[:, None] == jnp.arange(8, dtype=jnp.int32)[None, :]
    ).astype(jnp.float32)
    return jnp.sum(blocks[:, :, None] * onehot[:, None, :], axis=0)


def rows_to_windows(values, tiles):
    lon = values.shape[0]
    halves = values.reshape(2, lon // 2, *values.shape[1:])
    odd = lax.axis_index(SEC_TILE) % 2 == 1
    straight, crossed = half_routes(tiles)
    first = lax.ppermute(jnp.where(odd, halves[1], halves[0]), SEC_TILE, straight)
    second = lax.ppermute(jnp.where(odd, halves[0], halves[1]), SEC_TILE, crossed)
    east = lax.axis_index("sec") == 1
    pair = jnp.stack([jnp.where(east, second, first), jnp.where(east, first, second)])
    parts = [
        shift_tiles(pair, 1, tiles),
        pair,
        shift_tiles(pair, -1, tiles),
        shift_tiles(pair, -2, tiles),
    ]
    return jnp.concatenate(parts, axis=0)


def windows_to_rows(parts, tiles):
    pair = (
        parts[2:4]
        + shift_tiles(parts[0:2], -1, tiles)
        + shift_tiles(parts[4:6], 1, tiles)
        + shift_tiles(parts[6:8], 2, tiles)
    )
    east = lax.axis_index("sec") == 1
    straight, crossed = half_routes(tiles)
    first = lax.ppermute(jnp.where(east, pair[1], pair[0]), SEC_TILE, back(straight))
    second = lax.ppermute(jnp.where(east, pair[0], pair[1]), SEC_TILE, back(crossed))
    odd = lax.axis_index(SEC_TILE) % 2 == 1
    return jnp.concatenate([jnp.where(odd, second, first), jnp.where(odd, first, second)])


def coupled_window(
    atmosphere,
    ocean_state,
    land_mask,
    crossing_bands,
    ocean_regrid,
    atmosphere_regrid,
    surface_read,
    surface_embed,
    flux_read,
    flux_embed,
    legendre_forward,
    legendre_inverse,
    spectral_mix,
    conv_kernel,
    norm_gain,
    expand_weight,
    project_weight,
    atmosphere_cotangent,
    ocean_cotangent,
):
    band_total = lax.axis_size(SEC_TILE)
    _, lon_count, _ = atmosphere.shape
    ocean_rows, ocean_lon, ocean_channels = ocean_state.shape
    half = lon_count // lax.axis_size("sec")
    ratio = ocean_lon // half
    flux_count = flux_read.shape[1]
    radius = conv_kernel.shape[1] // 2
    highest = lax.Precision.HIGHEST
    mask_value = land_mask.astype(jnp.float32)
    tiles = lax.axis_size(TILE)
    to_ocean = window_matrix(crossing_bands[0], ocean_regrid[0, :, :, 0])
    from_ocean = window_matrix(crossing_bands[0], atmosphere_regrid[0, :, 0, :])
    surface = jnp.dot(ocean_state, surface_read, preferred_element_type=jnp.float32)
    coarse = jnp.mean((mask_value * surface).reshape(ocean_rows, half, ratio), axis=2)
    surface_atmosphere = windows_to_rows(
        jnp.sum(from_ocean[:, :, None] * coarse[:, None, :], axis=0), tiles
    )[None]
    flux = jnp.einsum("agc,cf->agf", atmosphere, flux_read, preferred_element_type=jnp.float32)
    flux_window = rows_to_windows(flux[0], tiles)
    flux_ocean = jnp.dot(
        to_ocean, flux_window.reshape(flux_window.shape[0], half * flux_count), precision=highest
    )
    mixed_input = (
        atmosphere.astype(jnp.float32)
        + surface_atmosphere[:, :, None] * surface_embed[None, None, :]
    ).astype(jnp.bfloat16)
    table = wave_table(lon_count, legendre_forward.shape[0] * band_total)
    spectrum = jnp.einsum(
        "gk,agc->akc", table, mixed_input, preferred_element_type=jnp.float32
    ).astype(jnp.bfloat16)
    returned = to_bands(
        spectral_block(to_modes(spectrum), legendre_forward, legendre_inverse, spectral_mix),
    )
    response = jnp.einsum("gk,akc->agc", table, returned, preferred_element_type=jnp.float32)
    atmosphere_next = (mixed_input.astype(jnp.float32) + jax.nn.gelu(response)).astype(jnp.bfloat16)
    forcing_coarse = jnp.einsum(
        "ogf,fc->ogc",
        flux_ocean.reshape(ocean_rows, half, flux_count),
        flux_embed.astype(jnp.float32),
        precision=highest,
    )
    forcing = jnp.broadcast_to(
        forcing_coarse[:, :, None, :], (ocean_rows, half, ratio, ocean_channels)
    ).reshape(ocean_rows, ocean_lon, ocean_channels)
    state = (ocean_state.astype(jnp.float32) + mask_value[:, :, None] * forcing).astype(
        jnp.bfloat16
    )
    side = conv_kernel.shape[1]
    taps = conv_kernel.astype(jnp.float32).reshape(conv_kernel.shape[0], side * side, -1)
    wet = jnp.broadcast_to(land_mask[:, :, None], ocean_state.shape).astype(jnp.bfloat16)
    gains = norm_gain[:, None, :]
    expand_t = jnp.swapaxes(expand_weight, 1, 2)
    project_t = jnp.swapaxes(project_weight, 1, 2)
    tile_out = chunked(ocean_rows, ocean_lon, ocean_channels, jnp.bfloat16)
    wide_out = chunked(ocean_rows, ocean_lon, ocean_channels, jnp.float32)
    rim_out = chunked(radius, ocean_lon, ocean_channels, jnp.bfloat16)
    cells = ocean_rows * ocean_lon
    work = 2 * cells * ocean_channels * side * side
    product = 2 * cells * ocean_channels * expand_weight.shape[2]
    state_1, near_1, far_1, hidden_0 = ocean_call(
        forward_kernel,
        rim_pieces(
            state,
            send_rows(state, radius, True),
            send_rows(state, radius, False),
            radius,
            tiles,
        ),
        (taps[0], gains[0], expand_weight[0], project_weight[0]),
        (wet,),
        [tile_out, rim_out, rim_out, wide_out],
        side,
        work + 2 * product,
    )
    state_2, adjoint_1, near_2, far_2 = ocean_call(
        turn_kernel,
        rim_pieces(state_1, near_1, far_1, radius, tiles),
        (
            taps[1],
            gains[1],
            expand_weight[1],
            project_weight[1],
            expand_t[1],
            project_t[1],
        ),
        (wet, ocean_cotangent),
        [tile_out, tile_out, rim_out, rim_out],
        side,
        work + 4 * product,
        1,
    )
    cotangent_1, adjoint_0, near_3, far_3 = ocean_call(
        backward_kernel,
        rim_pieces(adjoint_1, near_2, far_2, radius, tiles),
        (
            taps[1],
            gains[0],
            expand_weight[0],
            expand_t[0],
            project_t[0],
        ),
        (wet, ocean_cotangent, hidden_0),
        [wide_out, tile_out, rim_out, rim_out],
        side,
        work + 3 * product,
    )
    steps = ocean_lon // CHUNK
    coarse_chunk = CHUNK // ratio
    gather = (
        jnp.arange(ocean_rows * coarse_chunk, dtype=jnp.int32)[:, None]
        == jnp.arange(ocean_rows * CHUNK, dtype=jnp.int32)[None, :] // ratio
    ).astype(jnp.bfloat16)
    cotangent_0, flux_blocks = ocean_call(
        last_kernel,
        rim_pieces(adjoint_0, near_3, far_3, radius, tiles),
        (
            taps[0],
            gather,
            flux_embed.T,
        ),
        (wet, cotangent_1),
        [
            wide_out,
            stepped(steps, ocean_rows * coarse_chunk, flux_count, jnp.float32),
        ],
        side,
        work,
    )
    atmosphere_adjoint = atmosphere_cotangent.astype(jnp.float32)
    _, gelu_back = jax.vjp(jax.nn.gelu, response)
    response_adjoint = gelu_back(atmosphere_adjoint)[0].astype(jnp.bfloat16)
    returned_adjoint = jnp.einsum(
        "gk,agc->akc", table, response_adjoint, preferred_element_type=jnp.float32
    ).astype(jnp.bfloat16)
    spectrum_adjoint = to_bands(
        spectral_adjoint(
            to_modes(returned_adjoint), legendre_forward, legendre_inverse, spectral_mix
        ),
    )
    input_adjoint = atmosphere_adjoint + jnp.einsum(
        "gk,akc->agc", table, spectrum_adjoint, preferred_element_type=jnp.float32
    )
    surface_adjoint = jnp.einsum("agc,c->ag", input_adjoint, surface_embed, precision=highest)
    coarse_adjoint = jnp.dot(
        from_ocean, rows_to_windows(surface_adjoint[0], tiles), precision=highest
    )
    coarse_blocks = (
        jnp.swapaxes((coarse_adjoint / ratio).reshape(ocean_rows, steps, coarse_chunk), 0, 1)
    ).reshape(steps, ocean_rows * coarse_chunk, 1)
    ocean_grad = surface_call(
        gather.T, surface_read.astype(jnp.float32)[None, :], coarse_blocks, wet, cotangent_0
    )
    flux_ocean_adjoint = jnp.swapaxes(
        flux_blocks.reshape(steps, ocean_rows, coarse_chunk, flux_count), 0, 1
    ).reshape(ocean_rows, half, flux_count)
    flux_parts = jnp.dot(
        to_ocean.T, flux_ocean_adjoint.reshape(ocean_rows, half * flux_count), precision=highest
    )
    flux_adjoint = windows_to_rows(
        flux_parts.reshape(flux_parts.shape[0], half, flux_count), tiles
    )[None]
    from_flux = jnp.einsum(
        "agf,cf->agc", flux_adjoint, flux_read.astype(jnp.float32), precision=highest
    )
    atmosphere_grad = input_adjoint + from_flux
    return (atmosphere_next, state_2, atmosphere_grad, ocean_grad)


def solution(mesh):
    finer = Mesh(
        mesh.devices.reshape(mesh.shape["sec"], 4, 2, 4, 2),
        ("sec", "tile_0", "tile_1", "tile_2", "tile_3"),
    )
    placed = (
        P(SEC_TILE, None, None),
        P(TILE, "sec", None),
        P(TILE, "sec"),
        P(TILE, None),
        P(TILE, None, None, None),
        P(TILE, None, None, None),
        P(),
        P(),
        P(),
        P(),
        P(SEC_TILE, None, None),
        P(SEC_TILE, None, None),
        P(),
        P(),
        P(),
        P(),
        P(),
        P(SEC_TILE, None, None),
        P(TILE, "sec", None),
    )
    return jax.shard_map(
        coupled_window,
        mesh=finer,
        in_specs=placed,
        out_specs=(
            P(SEC_TILE, None, None),
            P(TILE, "sec", None),
            P(SEC_TILE, None, None),
            P(TILE, "sec", None),
        ),
        check_vma=False,
    )
```
